16 devices in a mesh: dp: 4 (over y, z, core), tp: 4 (over x).
Axes of the slice: x: 4, y: 2, z: 1, core: 2. Of those that a mesh axis runs over, the one named last changes fastest.
The devices are a block of a 4x4x4 slice.
Arguments:
- x: bfloat16 [256, 4096], P('dp'), parts along dimension 0
- k_cache: bfloat16 [256, 1024, 64, 64], P('dp', None, 'tp'), parts along dimension 0
- v_cache: bfloat16 [256, 1024, 64, 64], P('dp', None, 'tp'), parts along dimension 0
- gain_a: bfloat16 [4096], replicated
- wq: bfloat16 [4096, 4096], P(None, 'tp')
- wo: bfloat16 [4096, 4096], P('tp')
- gain_m: bfloat16 [4096], replicated
- w_gate: bfloat16 [4096, 10240], P(None, 'tp')
- w_up: bfloat16 [4096, 10240], P(None, 'tp')
- w_down: bfloat16 [10240, 4096], P('tp')
Outputs:
- output: bfloat16 [256, 4096], P('dp'), parts along dimension 0
There are 4 independent parts. The reference program is written for one: setup_inputs(seed, part) draws one part's arguments, and reference() takes and returns one part's arrays. A program takes and returns all parts, laid end to end along the dimension named above; an argument that names none is the same for every part.
All inputs are finite; a program needn't handle non-finite values.
Results may differ from the reference program's by a relative error of at most 0.017.
Values are sent between devices in bfloat16 or wider.
A program may use at most 1.5 GiB of HBM per device.

```python
import jax
import jax.numpy as jnp
from jax import lax

BATCH = 64
CACHE = 1024
D = 4096
HEADS = 64
KV_HEADS = 64
HEAD = 64
FF = 10240
THETA = 10000


def setup_inputs(seed: int = 0, part: int = 0) -> dict:
    kx, kc, kw, kn, kq, ko, km, kg, ku, kd = jax.random.split(jax.random.key(seed), 10)
    kx, kc, kw = (jax.random.fold_in(k, part) for k in (kx, kc, kw))

    def weights(key, rows, columns):
        return jax.random.normal(key, (rows, columns), jnp.float32) * rows**-0.5

    drawn = {
        "x": jax.random.normal(kx, (BATCH, D), jnp.float32),
        "k_cache": 2 * jax.random.normal(kc, (BATCH, CACHE, KV_HEADS, HEAD), jnp.float32),
        "v_cache": 4 * jax.random.normal(kw, (BATCH, CACHE, KV_HEADS, HEAD), jnp.float32),
        "gain_a": 1 + 0.1 * jax.random.normal(kn, (D,), jnp.float32),
        "wq": 2 * weights(kq, D, HEADS * HEAD),
        "wo": weights(ko, HEADS * HEAD, D),
        "gain_m": 1 + 0.1 * jax.random.normal(km, (D,), jnp.float32),
        "w_gate": weights(kg, D, FF),
        "w_up": weights(ku, D, FF),
        "w_down": 2 * weights(kd, FF, D),
    }
    return {k: v.astype(jnp.bfloat16) for k, v in drawn.items()}


def normed(x, gain):
    wide = x.astype(jnp.float32)
    scale = lax.rsqrt(jnp.mean(wide * wide, -1, keepdims=True) + 1e-6)
    return (wide * scale * gain.astype(jnp.float32)).astype(jnp.bfloat16)


def turned(t, place, theta):
    half = t.shape[-1] // 2
    angle = place.astype(jnp.float32)[:, None] * theta ** (-jnp.arange(half, dtype=jnp.float32) / half)
    cos, sin = jnp.cos(angle)[:, None], jnp.sin(angle)[:, None]
    a, b = t[..., :half].astype(jnp.float32), t[..., half:].astype(jnp.float32)
    return jnp.concatenate([a * cos - b * sin, b * cos + a * sin], -1).astype(jnp.bfloat16)


def matmul(a, w):
    return jnp.dot(a, w, preferred_element_type=jnp.float32).astype(jnp.bfloat16)


def einsum(form, a, b):
    return jnp.einsum(form, a.astype(jnp.float32), b.astype(jnp.float32))


def seen_by(a, wq, k_cache, v_cache, head, theta):
    batch, cache, kv_heads = k_cache.shape[:3]
    place = jnp.full((batch,), cache - 1)
    q = turned(matmul(a, wq).reshape(batch, -1, head), place, theta).reshape(batch, kv_heads, -1, head)
    scores = einsum("bgsd,bugd->bgsu", q, k_cache) * head**-0.5
    weights = jax.nn.softmax(scores, -1).astype(jnp.bfloat16)
    return einsum("bgsu,bugd->bgsd", weights, v_cache).astype(jnp.bfloat16).reshape(batch, -1)


def hidden_of(b, w_gate, w_up):
    gate = jnp.dot(b, w_gate, preferred_element_type=jnp.float32)
    up = jnp.dot(b, w_up, preferred_element_type=jnp.float32)
    return (jax.nn.silu(gate) * up).astype(jnp.bfloat16)


def reference(x, k_cache, v_cache, gain_a, wq, wo, gain_m, w_gate, w_up, w_down):
    seen = seen_by(normed(x, gain_a), wq, k_cache, v_cache, HEAD, THETA)
    h = (x.astype(jnp.float32) + jnp.dot(seen, wo, preferred_element_type=jnp.float32)).astype(jnp.bfloat16)
    hidden = hidden_of(normed(h, gain_m), w_gate, w_up)
    return (h.astype(jnp.float32) + jnp.dot(hidden, w_down, preferred_element_type=jnp.float32)).astype(jnp.bfloat16)
```

```python
import functools

import jax
import jax.numpy as jnp
import numpy as np
from jax import lax
from jax.experimental import pallas as pl
from jax.experimental.pallas import tpu as pltpu
from jax.sharding import PartitionSpec as P

HEAD = 64
THETA = 10000
T = 1024
NB = 6
G = 16
EARLY = 10

F32, BF16 = jnp.float32, jnp.bfloat16
MESH = pl.DeviceIdType.MESH


def dot(a, b):
    return jnp.dot(a, b, preferred_element_type=F32)


def kernel(
    n, x_hbm, k_hbm, v_hbm, ga_hbm, wq_hbm, wo_hbm, gm_hbm, wg_hbm, wu_hbm, wd_hbm, rot_hbm, out_hbm,
    tiles, x_ref, a_ref, h_ref, q_ref, s_ref, attn_ref, gain_ref, rot_ref, terms, acc_ref, hidden_ref, sums, got, y_ref,
    small_sem, wq_sem, k_sem, v_sem, wo_sem, mlp_sem, t_send, t_recv, s_send, s_recv, y_send, y_recv, out_sem,
):
    me = lax.axis_index("tp")
    batch, d = x_hbm.shape
    width = wq_hbm.shape[1]
    ff = wg_hbm.shape[1]
    heads = width // HEAD
    half = T // 2
    nq, no, nk, nc = d // T, d // T, d // T, ff // half
    ngu = nc * nk
    nd = ff * d // (T * T)
    wq_at = 2 * NB + no
    groups = batch // G

    def peer(i):
        return lax.rem(me + i, n)

    def source(i):
        return lax.rem(me + n - i, n)

    small = [
        pltpu.make_async_copy(s, t, small_sem.at[i])
        for i, (s, t) in enumerate([(x_hbm, x_ref), (ga_hbm, gain_ref.at[0]), (gm_hbm, gain_ref.at[1]), (rot_hbm, rot_ref)])
    ]
    wq = [pltpu.make_async_copy(wq_hbm.at[pl.ds(i * T, T)], tiles.at[wq_at + i], wq_sem.at[i]) for i in range(nq)]
    wo = [pltpu.make_async_copy(wo_hbm.at[:, pl.ds(i * T, T)], tiles.at[2 * NB + i], wo_sem.at[i]) for i in range(no)]

    def keys(b):
        p = lax.rem(b, NB)
        return pltpu.make_async_copy(k_hbm.at[b], tiles.at[2 * p], k_sem.at[p])

    def values(b):
        p = lax.rem(b, NB)
        return pltpu.make_async_copy(v_hbm.at[b], tiles.at[2 * p + 1], v_sem.at[p])

    def gate_up(j, at):
        c, k = j // nk, j % nk
        rows, columns = pl.ds(k * T, T), pl.ds(pl.multiple_of(c * half, half), half)
        return [
            pltpu.make_async_copy(w.at[rows, columns], tiles.at[at, :, pl.ds(i * half, half)], mlp_sem.at[j, i])
            for i, w in enumerate((wg_hbm, wu_hbm))
        ]

    def down(j, at):
        copies = []
        for i in range(2):
            t, r = divmod(2 * j + i, nc)
            columns = pl.ds(pl.multiple_of(peer(1 + t) * T, T), T)
            copies.append(
                pltpu.make_async_copy(wd_hbm.at[pl.ds(r * half, half), columns], tiles.at[at, pl.ds(i * half, half)], mlp_sem.at[ngu + j, i])
            )
        return copies

    freed = [s for b in range(batch - NB, batch) for s in (2 * (b % NB), 2 * (b % NB) + 1)]
    place = [wq_at + j for j in range(EARLY)] + freed + [2 * NB + j for j in range(no)]
    place += [wq_at + j for j in range(ngu + nd - len(place))]

    def mlp(j):
        return gate_up(j, place[j]) if j < ngu else down(j - ngu, place[j])

    def start(copies):
        for c in copies:
            c.start()

    def wait(copies):
        for c in copies:
            c.wait()

    start(small)
    start(wq)
    for b in range(NB):
        keys(b).start()
        values(b).start()
    start(wo)

    barrier = pltpu.get_barrier_semaphore()
    for i in range(1, n):
        pl.semaphore_signal(barrier, inc=1, device_id={"tp": peer(i)}, device_id_type=MESH)
    pl.semaphore_wait(barrier, n - 1)

    def normed(rows, wide, gain):
        scale = lax.rsqrt(jnp.mean(wide * wide, -1, keepdims=True) + 1e-6)
        a_ref[rows, :] = (wide * scale * gain_ref[gain].astype(F32)).astype(BF16)

    wait(small)

    @pl.loop(0, batch // G)
    def _(g):
        rows = pl.ds(pl.multiple_of(g * G, G), G)
        normed(rows, x_ref[rows, :].astype(F32), 0)

    q = None
    for i in range(nq):
        wq[i].wait()
        part = dot(a_ref[:, i * T : (i + 1) * T], tiles[wq_at + i])
        q = part if q is None else q + part
    q = q.astype(BF16).astype(F32)
    lane = lax.broadcasted_iota(jnp.int32, q.shape, 1)
    other = jnp.where(lane % HEAD < HEAD // 2, pltpu.roll(q, width - HEAD // 2, 1), pltpu.roll(q, HEAD // 2, 1))
    q_ref[...] = (q * rot_ref[0:1, :] + other * rot_ref[1:2, :]).astype(BF16).astype(F32)

    own = lax.broadcasted_iota(jnp.int32, (heads, width), 1) // HEAD == lax.broadcasted_iota(jnp.int32, (heads, width), 0)

    def scores(b):
        q = jnp.where(own, jnp.broadcast_to(q_ref[pl.ds(b, 1), :], (heads, width)), 0.0).astype(BF16)
        return dot(q, tiles[2 * lax.rem(b, NB)])

    def sends(g):
        return [
            pltpu.make_async_remote_copy(
                terms.at[g, me], terms.at[g, me], t_send.at[g, i - 1], t_recv.at[g, i - 1], device_id={"tp": peer(i)}, device_id_type=MESH
            )
            for i in range(1, n)
        ]

    def receives(g):
        return [
            pltpu.make_async_remote_copy(
                terms.at[g, source(i)], terms.at[g, source(i)], t_send.at[g, i - 1], t_recv.at[g, i - 1], device_id={"tp": peer(i)}, device_id_type=MESH
            )
            for i in range(1, n)
        ]

    def finish(g):
        for c in sends(g):
            c.wait_send()
        for c in receives(g):
            c.wait_recv()
        rows = pl.ds(pl.multiple_of(g * G, G), G)
        total = terms[g, 0].astype(F32)
        for i in range(1, n):
            total = total + terms[g, i].astype(F32)
        h = (x_ref[rows, :].astype(F32) + total).astype(BF16)
        h_ref[rows, :] = h
        normed(rows, h.astype(F32), 1)

    keys(0).wait()
    s_ref[...] = scores(0)

    @pl.loop(0, batch)
    def _(b):
        values(b).wait()

        @pl.when(b + 1 < batch)
        def _():
            keys(b + 1).wait()

        later = scores(jnp.minimum(b + 1, batch - 1))
        s = s_ref[...] * HEAD**-0.5
        e = jnp.exp(s - jnp.max(s, -1, keepdims=True))
        w = (e / jnp.sum(e, -1, keepdims=True)).astype(BF16)
        r = lax.dot_general(w, tiles[2 * lax.rem(b, NB) + 1], (((1,), (1,)), ((), ())), preferred_element_type=F32)
        attn_ref[pl.ds(b, 1), :] = jnp.sum(jnp.where(own, r, 0.0), 0, keepdims=True)
        s_ref[...] = later

        @pl.when(b + NB < batch)
        def _():
            keys(b + NB).start()
            values(b + NB).start()

        @pl.when(b == batch - NB - 1)
        def _():
            for j in range(EARLY):
                start(mlp(j))

        @pl.when(jnp.logical_and(b >= batch - NB, b < batch - NB + (ngu - EARLY) // 2))
        def _():
            for i in range(2):
                start(gate_up(EARLY + 2 * (b - (batch - NB)) + i, 2 * lax.rem(b, NB) + i))

        @pl.when(lax.rem(b, G) == G - 1)
        def _():
            g = b // G

            @pl.when(g == 0)
            def _():
                wait(wo)

            part = attn_ref[pl.ds(pl.multiple_of(g * G, G), G), :].astype(BF16)
            for i in range(no):
                terms[g, me, :, i * T : (i + 1) * T] = dot(part, tiles[2 * NB + i]).astype(BF16)
            start(sends(g))

            @pl.when(g > 0)
            def _():
                finish(g - 1)

    for j in range(ngu, EARLY + 2 * NB + no):
        start(mlp(j))
    finish(groups - 1)

    for c in range(nc):
        for k in range(nk):
            j = c * nk + k
            wait(mlp(j))
            part = dot(a_ref[:, k * T : (k + 1) * T], tiles[place[j]])
            if k == 0:
                acc_ref[...] = part
            else:
                acc_ref[...] += part
            if j + EARLY + 2 * NB + no < ngu + nd:
                start(mlp(j + EARLY + 2 * NB + no))
        gate, up = acc_ref[:, :half], acc_ref[:, half:]
        hidden_ref[:, c * half : (c + 1) * half] = (gate * jax.nn.sigmoid(gate) * up).astype(BF16)

    for t in range(n):
        total = None
        for r in range(nc):
            j, i = divmod(t * nc + r, 2)
            if i == 0 or r == 0 and t == 0:
                wait(down(j, place[ngu + j]))
            part = dot(hidden_ref[:, r * half : (r + 1) * half], tiles[place[ngu + j], i * half : (i + 1) * half])
            total = part if total is None else total + part
        if t < n - 1:
            sums[t] = total.astype(BF16)
            pltpu.make_async_remote_copy(
                sums.at[t], got.at[t], s_send.at[t], s_recv.at[t], device_id={"tp": peer(1 + t)}, device_id_type=MESH
            ).start()
    mine = pl.ds(pl.multiple_of(me * T, T), T)
    for t in range(n - 1):
        copy = pltpu.make_async_remote_copy(
            sums.at[t], got.at[t], s_send.at[t], s_recv.at[t], device_id={"tp": peer(1 + t)}, device_id_type=MESH
        )
        copy.wait()
        total = total + got[t].astype(F32)
    y_ref[...] = (h_ref[:, mine].astype(F32) + total).astype(BF16)
    ys = [
        pltpu.make_async_remote_copy(
            y_ref, out_hbm.at[:, mine], y_send.at[i - 1], y_recv.at[i - 1], device_id={"tp": peer(i)}, device_id_type=MESH
        )
        for i in range(1, n)
    ]
    start(ys)
    here = pltpu.make_async_copy(y_ref, out_hbm.at[:, mine], out_sem)
    here.start()
    here.wait()
    for i in range(1, n):
        ys[i - 1].wait_send()
        theirs = pl.ds(pl.multiple_of(source(i) * T, T), T)
        pltpu.make_async_remote_copy(
            y_ref, out_hbm.at[:, theirs], y_send.at[i - 1], y_recv.at[i - 1], device_id={"tp": peer(i)}, device_id_type=MESH
        ).wait_recv()


def solution(mesh):
    n = mesh.shape["tp"]

    def step(x, k_cache, v_cache, gain_a, wq, wo, gain_m, w_gate, w_up, w_down):
        batch, cache, heads, head = k_cache.shape
        d, width = wq.shape
        ff = w_gate.shape[1]
        k = jnp.transpose(k_cache, (0, 2, 3, 1)).reshape(batch, width, cache)
        v = jnp.transpose(v_cache, (0, 2, 3, 1)).reshape(batch, width, cache)
        angle = np.float32(cache - 1) * np.float32(THETA) ** (-np.arange(head // 2, dtype=np.float32) / np.float32(head // 2))
        cos, sin = np.cos(angle), np.sin(angle)
        rot = np.stack([np.tile(np.concatenate(c), heads) for c in ((cos, cos), (-sin, sin))]).astype(np.float32)
        no, nd, ngu = d // T, ff * d // (T * T), 2 * ff * d // (T * T)
        groups = batch // G
        dma = pltpu.SemaphoreType.DMA
        anywhere = pl.BlockSpec(memory_space=pl.ANY)
        return pl.pallas_call(
            functools.partial(kernel, n),
            out_shape=jax.ShapeDtypeStruct((batch, d), BF16),
            in_specs=[anywhere] * 11,
            out_specs=anywhere,
            scratch_shapes=[
                pltpu.VMEM((2 * NB + no + EARLY, T, T), BF16),
                pltpu.VMEM((batch, d), BF16),
                pltpu.VMEM((batch, d), BF16),
                pltpu.VMEM((batch, d), BF16),
                pltpu.VMEM((batch, width), F32),
                pltpu.VMEM((heads, cache), F32),
                pltpu.VMEM((batch, width), F32),
                pltpu.VMEM((2, 1, d), BF16),
                pltpu.VMEM((2, width), F32),
                pltpu.VMEM((groups, n, G, d), BF16),
                pltpu.VMEM((batch, T), F32),
                pltpu.VMEM((batch, ff), BF16),
                pltpu.VMEM((n - 1, batch, T), BF16),
                pltpu.VMEM((n - 1, batch, T), BF16),
                pltpu.VMEM((batch, T), BF16),
                dma((4,)), dma((d // T,)), dma((NB,)), dma((NB,)), dma((no,)), dma((ngu + nd, 2)),
                dma((groups, n - 1)), dma((groups, n - 1)), dma((n - 1,)), dma((n - 1,)), dma((n - 1,)), dma((n - 1,)), dma,
            ],
            compiler_params=pltpu.CompilerParams(collective_id=0, has_side_effects=True, vmem_limit_bytes=67043328),
            name="layer",
        )(x, k, v, gain_a.reshape(1, d), wq, wo, gain_m.reshape(1, d), w_gate, w_up, w_down, rot)

    states, cache, columns, rows_of = P("dp", None), P("dp", None, "tp", None), P(None, "tp"), P("tp", None)
    return jax.shard_map(
        step,
        mesh=mesh,
        in_specs=(states, cache, cache, P(None), columns, rows_of, P(None), columns, columns, rows_of),
        out_specs=states,
        check_vma=False,
    )
```

```python
import functools

import jax
import jax.numpy as jnp
import numpy as np
from jax import lax
from jax.experimental import pallas as pl
from jax.experimental.pallas import tpu as pltpu
from jax.sharding import PartitionSpec as P

HEAD = 64
THETA = 10000
T = 1024
AHEAD = 4
NB = AHEAD + 1
G = 8
EARLY = 12

F32, BF16 = jnp.float32, jnp.bfloat16
MESH = pl.DeviceIdType.MESH


def dot(a, b):
    return jnp.dot(a, b, preferred_element_type=F32)


def few(a, b):
    return dot(jnp.concatenate([a, a], 0), b)


def kernel(
    n, x_hbm, k_hbm, v_hbm, ga_hbm, wq_hbm, wo_hbm, gm_hbm, wg_hbm, wu_hbm, wd_hbm, rot_hbm, out_ref,
    tiles, x_ref, a_ref, h_ref, normed_ref, q_ref, s_ref, attn_ref, gain_ref, wide_gain, rot_ref, terms, hidden_ref, sums, passing, waiting, got,
    small_sem, wq_sem, k_sem, v_sem, wo_sem, mlp_sem, t_send, t_recv, p_send, p_recv, s_send, s_recv, y_send, y_recv,
):
    me = lax.axis_index("tp")
    batch, d = x_hbm.shape
    width = wq_hbm.shape[1]
    ff = wg_hbm.shape[1]
    heads = width // HEAD
    half = T // 2
    nq, no, nk, nc = d // T, d // T, d // T, ff // half
    ngu = nc * nk
    nd = ff * d // (T * T)
    turns = (2, 1, n - 1, 0)
    wq_at = 2 * NB + no
    groups = batch // G

    def peer(i):
        return lax.rem(me + i, n)

    def source(i):
        return lax.rem(me + n - i, n)

    small = [
        pltpu.make_async_copy(s, t, small_sem.at[i])
        for i, (s, t) in enumerate([(x_hbm, x_ref), (ga_hbm, gain_ref.at[0]), (gm_hbm, gain_ref.at[1]), (rot_hbm, rot_ref)])
    ]
    wq = [pltpu.make_async_copy(wq_hbm.at[pl.ds(i * T, T)], tiles.at[wq_at + i], wq_sem.at[i]) for i in range(nq)]
    wo = [pltpu.make_async_copy(wo_hbm.at[:, pl.ds(i * T, T)], tiles.at[2 * NB + i], wo_sem.at[i]) for i in range(no)]

    def keys(b):
        p = lax.rem(b, NB)
        return pltpu.make_async_copy(k_hbm.at[b], tiles.at[2 * p], k_sem.at[p])

    def values(b):
        p = lax.rem(b, NB)
        return pltpu.make_async_copy(v_hbm.at[b], tiles.at[2 * p + 1], v_sem.at[p])

    def gate_up(j, at):
        c, k = j // nk, j % nk
        rows, columns = pl.ds(k * T, T), pl.ds(pl.multiple_of(c * half, half), half)
        return [
            pltpu.make_async_copy(w.at[rows, columns], tiles.at[at, :, pl.ds(i * half, half)], mlp_sem.at[j, i])
            for i, w in enumerate((wg_hbm, wu_hbm))
        ]

    def down(j, at):
        copies = []
        for i in range(2):
            t, r = divmod(2 * j + i, nc)
            columns = pl.ds(pl.multiple_of(peer(turns[t]) * T, T), T)
            copies.append(
                pltpu.make_async_copy(wd_hbm.at[pl.ds(r * half, half), columns], tiles.at[at, pl.ds(i * half, half)], mlp_sem.at[ngu + j, i])
            )
        return copies

    freed = [s for b in range(batch - NB, batch) for s in (2 * (b % NB), 2 * (b % NB) + 1)]
    place = [wq_at + j for j in range(EARLY)] + freed + [2 * NB + j for j in range(no)]
    place += [wq_at + j for j in range(ngu + nd - len(place))]

    def mlp(j):
        return gate_up(j, place[j]) if j < ngu else down(j - ngu, place[j])

    def start(copies):
        for c in copies:
            c.start()

    def wait(copies):
        for c in copies:
            c.wait()

    start(small)
    start(wq)

    barrier = pltpu.get_barrier_semaphore()
    for i in range(1, n):
        pl.semaphore_signal(barrier, inc=1, device_id={"tp": peer(i)}, device_id_type=MESH)

    def normed(wide, gain, to, rows):
        scale = lax.rsqrt(jnp.mean(wide * wide, -1, keepdims=True) + 1e-6)
        for c in range(d // 128):
            at = slice(c * 128, (c + 1) * 128)
            to[rows, at] = (wide[:, at] * scale * wide_gain[gain, c : c + 1, :]).astype(to.dtype)

    wait(small)
    for b in range(2):
        keys(b).start()
        values(b).start()
    wide_gain[...] = gain_ref[...].astype(F32)

    @pl.loop(0, batch // 16)
    def _(g):
        rows = pl.ds(pl.multiple_of(g * 16, 16), 16)
        wide = x_ref[rows, :].astype(F32)
        h_ref[rows, :] = wide
        normed(wide, 0, a_ref, rows)

    q = None
    for b in range(2, AHEAD):
        keys(b).start()
        values(b).start()
    for i in range(nq):
        wq[i].wait()
        part = dot(a_ref[:, i * T : (i + 1) * T], tiles[wq_at + i])
        q = part if q is None else q + part
    q = q.astype(BF16).astype(F32)
    lane = lax.broadcasted_iota(jnp.int32, q.shape, 1)
    other = jnp.where(lane % HEAD < HEAD // 2, pltpu.roll(q, width - HEAD // 2, 1), pltpu.roll(q, HEAD // 2, 1))
    q_ref[...] = (q * rot_ref[0:1, :] + other * rot_ref[1:2, :]).astype(BF16).astype(F32)

    own = lax.broadcasted_iota(jnp.int32, (heads, width), 1) // HEAD == lax.broadcasted_iota(jnp.int32, (heads, width), 0)

    def scores(b):
        q = jnp.where(own, jnp.broadcast_to(q_ref[pl.ds(b, 1), :], (heads, width)), 0.0).astype(BF16)
        return dot(q, tiles[2 * lax.rem(b, NB)])

    def sends(g):
        return [
            pltpu.make_async_remote_copy(
                terms.at[g, me], terms.at[g, me], t_send.at[g, i - 1], t_recv.at[g, i - 1], device_id={"tp": peer(i)}, device_id_type=MESH
            )
            for i in range(1, n)
        ]

    def receives(g):
        return [
            pltpu.make_async_remote_copy(
                terms.at[g, source(i)], terms.at[g, source(i)], t_send.at[g, i - 1], t_recv.at[g, i - 1], device_id={"tp": peer(i)}, device_id_type=MESH
            )
            for i in range(1, n)
        ]

    def finish(g):
        for c in sends(g):
            c.wait_send()
        for c in receives(g):
            c.wait_recv()
        rows = pl.ds(pl.multiple_of(g * G, G), G)
        total = terms[g, 0].astype(F32)
        for i in range(1, n):
            total = total + terms[g, i].astype(F32)
        h = (h_ref[rows, :] + total).astype(BF16).astype(F32)
        h_ref[rows, :] = h
        normed(h, 1, normed_ref, pl.ds(pl.multiple_of(lax.rem(g, 2) * G, G), G))

        @pl.when(lax.rem(g, 2) == 1)
        def _():
            a_ref[pl.ds(pl.multiple_of((g - 1) * G, 2 * G), 2 * G), :] = normed_ref[...].astype(BF16)

    pl.semaphore_wait(barrier, n - 1)
    keys(0).wait()
    s_ref[...] = scores(0)

    @pl.loop(0, batch)
    def _(b):
        @pl.when(b + AHEAD < batch)
        def _():
            keys(b + AHEAD).start()
            values(b + AHEAD).start()

        @pl.when(b < no)
        def _():
            pltpu.make_async_copy(
                wo_hbm.at[:, pl.ds(pl.multiple_of(b * T, T), T)], tiles.at[2 * NB + b], wo_sem.at[b]
            ).start()

        @pl.when(b >= batch - AHEAD)
        def _():
            for i in range(2):
                start(gate_up(2 * (b - (batch - AHEAD)) + i, wq_at + 2 * (b - (batch - AHEAD)) + i))

        values(b).wait()

        @pl.when(b + 1 < batch)
        def _():
            keys(b + 1).wait()

        later = scores(jnp.minimum(b + 1, batch - 1))
        s = s_ref[...] * HEAD**-0.5
        e = jnp.exp(s - jnp.max(s, -1, keepdims=True))
        w = (e / jnp.sum(e, -1, keepdims=True)).astype(BF16)
        r = lax.dot_general(w, tiles[2 * lax.rem(b, NB) + 1], (((1,), (1,)), ((), ())), preferred_element_type=F32)
        attn_ref[pl.ds(b, 1), :] = jnp.sum(jnp.where(own, r, 0.0), 0, keepdims=True)
        s_ref[...] = later

        @pl.when(lax.rem(b, G) == G - 1)
        def _():
            g = b // G

            @pl.when(g == 0)
            def _():
                wait(wo)

            part = attn_ref[pl.ds(pl.multiple_of(g * G, G), G), :].astype(BF16)
            for i in range(no):
                terms[g, me, :, i * T : (i + 1) * T] = dot(part, tiles[2 * NB + i]).astype(BF16)
            start(sends(g))

            @pl.when(g > 0)
            def _():
                finish(g - 1)

    for j in range(2 * AHEAD, EARLY + 2 * NB + no):
        start(mlp(j))
    finish(groups - 1)

    quarter = T // 4
    held = EARLY + 2 * NB + no
    for c in range(nc):
        js = range(c * nk, (c + 1) * nk)
        for j in js:
            wait(mlp(j))

        def product(i):
            product = sum(few(a_ref[:, k * T : (k + 1) * T], tiles[place[j], :, i * quarter : (i + 1) * quarter]) for k, j in enumerate(js))
            return product[:batch]

        for i in range(2):
            gate, up = product(i), product(2 + i)
            hidden_ref[:, c * half + i * quarter : c * half + (i + 1) * quarter] = (gate * jax.nn.sigmoid(gate) * up).astype(BF16)
        for j in js:
            if j + held < ngu + nd:
                start(mlp(j + held))

    right, left = peer(1), peer(n - 1)
    ways = (right, left)
    top, bottom = slice(0, batch // 2), slice(batch // 2, batch)
    halves = (top, bottom)

    def send(src, dst, send_sem, recv_sem, to):
        return pltpu.make_async_remote_copy(src, dst, send_sem, recv_sem, device_id={"tp": to}, device_id_type=MESH)

    passed = [send(sums.at[0, halves[w]], passing.at[w], p_send.at[w], p_recv.at[w], ways[w]) for w in range(2)]
    direct = [send(sums.at[1 + w, halves[1 - w]], got.at[w, halves[1 - w]], s_send.at[w, 0], s_recv.at[w, 0], ways[w]) for w in range(2)]
    added = [send(sums.at[1 + w, halves[w]], got.at[w, halves[w]], s_send.at[w, 1], s_recv.at[w, 1], ways[w]) for w in range(2)]
    waited = 0
    for t in range(n):
        blocks = [divmod(t * nc + r, 2) for r in range(nc)]
        while waited <= blocks[-1][0]:
            wait(down(waited, place[ngu + waited]))
            waited += 1
        for c in range(4):
            at = slice(c * quarter, (c + 1) * quarter)
            total = sum(
                few(hidden_ref[:, r * half : (r + 1) * half], tiles[place[ngu + j], i * half : (i + 1) * half, at]) for r, (j, i) in enumerate(blocks)
            )[:batch]
            if t == 0:
                sums[0, :, at] = total.astype(BF16)
            elif t < n - 1:
                sums[t, halves[2 - t], at] = total[halves[2 - t]].astype(BF16)
                waiting[t - 1, :, at] = total[halves[t - 1]]
            else:
                waiting[0, :, at], waiting[1, :, at] = total[top], total[bottom]
        if t == 0:
            start(passed)
        elif t < n - 1:
            direct[t - 1].start()
        if t == n - 2:
            for w in range(2):
                passed[w].wait()
                sums[1 + w, halves[w]] = (waiting[w] + passing[w].astype(F32)).astype(BF16)
                added[w].start()
    mine = pl.ds(pl.multiple_of(me * T, T), T)
    wait(direct)
    wait(added)
    for w in range(2):
        total = waiting[w] + got[0, halves[w]].astype(F32) + got[1, halves[w]].astype(F32)
        out_ref[halves[w], mine] = (h_ref[halves[w], mine] + total).astype(BF16)

    def shared(w, i, c, h):
        block = out_ref.at[halves[h], pl.ds(pl.multiple_of(c * T, T), T)]
        return send(block, block, y_send.at[w, i], y_recv.at[w, i], ways[w])

    first = [shared(w, 0, me, w) for w in range(2)]
    second = [shared(w, 1, me, 1 - w) for w in range(2)]
    third = [shared(w, 2, ways[1 - w], w) for w in range(2)]
    start(first)
    start(second)
    for w in range(2):
        shared(w, 0, ways[1 - w], w).wait_recv()
        third[w].start()
    for w in range(2):
        shared(w, 1, ways[1 - w], 1 - w).wait_recv()
        shared(w, 2, peer(2), w).wait_recv()
    for copy in first + second + third:
        copy.wait_send()


def solution(mesh):
    n = mesh.shape["tp"]

    def step(x, k_cache, v_cache, gain_a, wq, wo, gain_m, w_gate, w_up, w_down):
        batch, cache, heads, head = k_cache.shape
        d, width = wq.shape
        ff = w_gate.shape[1]
        k = jnp.transpose(k_cache, (0, 2, 3, 1)).reshape(batch, width, cache)
        v = jnp.transpose(v_cache, (0, 2, 3, 1)).reshape(batch, width, cache)
        angle = np.float32(cache - 1) * np.float32(THETA) ** (-np.arange(head // 2, dtype=np.float32) / np.float32(head // 2))
        cos, sin = np.cos(angle), np.sin(angle)
        rot = np.stack([np.tile(np.concatenate(c), heads) for c in ((cos, cos), (-sin, sin))]).astype(np.float32)
        no, nd, ngu = d // T, ff * d // (T * T), 2 * ff * d // (T * T)
        groups = batch // G
        dma = pltpu.SemaphoreType.DMA
        anywhere = pl.BlockSpec(memory_space=pl.ANY)
        return pl.pallas_call(
            functools.partial(kernel, n),
            out_shape=pltpu.VMEM((batch, d), BF16),
            in_specs=[anywhere] * 11,
            out_specs=pl.BlockSpec(memory_space=pltpu.VMEM),
            scratch_shapes=[
                pltpu.VMEM((2 * NB + no + EARLY, T, T), BF16),
                pltpu.VMEM((batch, d), BF16),
                pltpu.VMEM((batch, d), BF16),
                pltpu.VMEM((batch, d), F32),
                pltpu.VMEM((2 * G, d), F32),
                pltpu.VMEM((batch, width), F32),
                pltpu.VMEM((heads, cache), F32),
                pltpu.VMEM((batch, width), F32),
                pltpu.VMEM((2, d // 128, 128), BF16),
                pltpu.VMEM((2, d // 128, 128), F32),
                pltpu.VMEM((2, width), F32),
                pltpu.VMEM((groups, n, G, d), BF16),
                pltpu.VMEM((batch, ff), BF16),
                pltpu.VMEM((n - 1, batch, T), BF16),
                pltpu.VMEM((2, batch // 2, T), BF16),
                pltpu.VMEM((2, batch // 2, T), F32),
                pltpu.VMEM((2, batch, T), BF16),
                dma((4,)), dma((d // T,)), dma((NB,)), dma((NB,)), dma((no,)), dma((ngu + nd, 2)),
                dma((groups, n - 1)), dma((groups, n - 1)), dma((2,)), dma((2,)), dma((2, 2)), dma((2, 2)), dma((2, 3)), dma((2, 3)),
            ],
            compiler_params=pltpu.CompilerParams(collective_id=0, has_side_effects=True, vmem_limit_bytes=65011712),
            name="layer",
        )(x, k, v, gain_a.reshape(d // 128, 128), wq, wo, gain_m.reshape(d // 128, 128), w_gate, w_up, w_down, rot)

    states, cache, columns, rows_of = P("dp", None), P("dp", None, "tp", None), P(None, "tp"), P("tp", None)
    return jax.shard_map(
        step,
        mesh=mesh,
        in_specs=(states, cache, cache, P(None), columns, rows_of, P(None), columns, columns, rows_of),
        out_specs=states,
        check_vma=False,
    )
```

```python
import functools

import jax
import jax.numpy as jnp
import numpy as np
from jax import lax
from jax.experimental import pallas as pl
from jax.experimental.pallas import tpu as pltpu
from jax.sharding import PartitionSpec as P

HEAD = 64
THETA = 10000
T = 1024
AHEAD = 4
NB = AHEAD + 1
G = 8
EARLY = 12

F32, BF16 = jnp.float32, jnp.bfloat16
MESH = pl.DeviceIdType.MESH


def dot(a, b):
    return jnp.dot(a, b, preferred_element_type=F32)


def few(a, b):
    return dot(jnp.concatenate([a, a], 0), b)


def kernel(
    n, x_hbm, k_hbm, v_hbm, ga_hbm, wq_hbm, wo_hbm, gm_hbm, wg_hbm, wu_hbm, wd_hbm, rot_hbm, out_ref,
    tiles, x_ref, a_ref, h_ref, normed_ref, q_ref, s_ref, attn_ref, gain_ref, wide_gain, rot_ref, terms, hidden_ref, sums, own_sum, got,
    small_sem, wq_sem, k_sem, v_sem, wo_sem, mlp_sem, t_send, t_recv, s_send, s_recv, y_send, y_recv,
):
    me = lax.axis_index("tp")
    batch, d = x_hbm.shape
    width = wq_hbm.shape[1]
    ff = wg_hbm.shape[1]
    heads = width // HEAD
    half = T // 2
    nq, no, nk, nc = d // T, d // T, d // T, ff // half
    ngu = nc * nk
    nd = ff * d // (T * T)
    turns = (2, 1, n - 1, 0)
    order = [(0, 0), (1, 0), (0, 1), (0, 2), (0, 3), (1, 1), (1, 2), (1, 3)]
    wq_at = 2 * NB + no
    groups = batch // G

    def peer(i):
        return lax.rem(me + i, n)

    def source(i):
        return lax.rem(me + n - i, n)

    small = [
        pltpu.make_async_copy(s, t, small_sem.at[i])
        for i, (s, t) in enumerate([(x_hbm, x_ref), (ga_hbm, gain_ref.at[0]), (gm_hbm, gain_ref.at[1]), (rot_hbm, rot_ref)])
    ]
    wq = [pltpu.make_async_copy(wq_hbm.at[pl.ds(i * T, T)], tiles.at[wq_at + i], wq_sem.at[i]) for i in range(nq)]
    wo = [pltpu.make_async_copy(wo_hbm.at[:, pl.ds(i * T, T)], tiles.at[2 * NB + i], wo_sem.at[i]) for i in range(no)]

    def keys(b):
        p = lax.rem(b, NB)
        return pltpu.make_async_copy(k_hbm.at[b], tiles.at[2 * p], k_sem.at[p])

    def values(b):
        p = lax.rem(b, NB)
        return pltpu.make_async_copy(v_hbm.at[b], tiles.at[2 * p + 1], v_sem.at[p])

    def gate_up(j, at):
        c, k = j // nk, j % nk
        rows, columns = pl.ds(k * T, T), pl.ds(pl.multiple_of(c * half, half), half)
        return [
            pltpu.make_async_copy(w.at[rows, columns], tiles.at[at, :, pl.ds(i * half, half)], mlp_sem.at[j, i])
            for i, w in enumerate((wg_hbm, wu_hbm))
        ]

    def block(i):
        (s, t), r = order[i // nc], i % nc
        j, at = i // 4, (pl.ds(i % 4 // 2 * half, half), pl.ds(i % 2 * half, half))
        return j, at, (pl.ds(r * half, half), pl.ds(pl.multiple_of(peer(turns[t]) * T + s * half, half), half))

    def down(i):
        j, at, source = block(i)
        return pltpu.make_async_copy(wd_hbm.at[source], tiles.at[(place[ngu + j], *at)], mlp_sem.at[ngu + j, i % 4])

    freed = [s for b in range(batch - NB, batch) for s in (2 * (b % NB), 2 * (b % NB) + 1)]
    place = [wq_at + j for j in range(EARLY)] + freed + [2 * NB + j for j in range(no)]
    place += [wq_at + j for j in range(ngu + nd - len(place))]

    def mlp(j):
        return gate_up(j, place[j]) if j < ngu else [down(4 * (j - ngu) + i) for i in range(4)]

    def start(copies):
        for c in copies:
            c.start()

    def wait(copies):
        for c in copies:
            c.wait()

    start(small)
    start(wq)

    barrier = pltpu.get_barrier_semaphore()
    for i in range(1, n):
        pl.semaphore_signal(barrier, inc=1, device_id={"tp": peer(i)}, device_id_type=MESH)

    def normed(wide, gain, to, rows):
        scale = lax.rsqrt(jnp.mean(wide * wide, -1, keepdims=True) + 1e-6)
        for c in range(d // 128):
            at = slice(c * 128, (c + 1) * 128)
            to[rows, at] = (wide[:, at] * scale * wide_gain[gain, c : c + 1, :]).astype(to.dtype)

    wait(small)
    for b in range(2):
        keys(b).start()
        values(b).start()
    wide_gain[...] = gain_ref[...].astype(F32)

    @pl.loop(0, batch // 16)
    def _(g):
        rows = pl.ds(pl.multiple_of(g * 16, 16), 16)
        wide = x_ref[rows, :].astype(F32)
        h_ref[rows, :] = wide
        normed(wide, 0, a_ref, rows)

    q = None
    for b in range(2, AHEAD):
        keys(b).start()
        values(b).start()
    for i in range(nq):
        wq[i].wait()
        part = dot(a_ref[:, i * T : (i + 1) * T], tiles[wq_at + i])
        q = part if q is None else q + part
    q = q.astype(BF16).astype(F32)
    lane = lax.broadcasted_iota(jnp.int32, q.shape, 1)
    other = jnp.where(lane % HEAD < HEAD // 2, pltpu.roll(q, width - HEAD // 2, 1), pltpu.roll(q, HEAD // 2, 1))
    q_ref[...] = (q * rot_ref[0:1, :] + other * rot_ref[1:2, :]).astype(BF16).astype(F32)

    own = lax.broadcasted_iota(jnp.int32, (heads, width), 1) // HEAD == lax.broadcasted_iota(jnp.int32, (heads, width), 0)

    def scores(b):
        q = jnp.where(own, jnp.broadcast_to(q_ref[pl.ds(b, 1), :], (heads, width)), 0.0).astype(BF16)
        return dot(q, tiles[2 * lax.rem(b, NB)])

    def sends(g):
        return [
            pltpu.make_async_remote_copy(
                terms.at[g, me], terms.at[g, me], t_send.at[g, i - 1], t_recv.at[g, i - 1], device_id={"tp": peer(i)}, device_id_type=MESH
            )
            for i in range(1, n)
        ]

    def receives(g):
        return [
            pltpu.make_async_remote_copy(
                terms.at[g, source(i)], terms.at[g, source(i)], t_send.at[g, i - 1], t_recv.at[g, i - 1], device_id={"tp": peer(i)}, device_id_type=MESH
            )
            for i in range(1, n)
        ]

    def finish(g):
        for c in sends(g):
            c.wait_send()
        for c in receives(g):
            c.wait_recv()
        rows = pl.ds(pl.multiple_of(g * G, G), G)
        total = terms[g, 0].astype(F32)
        for i in range(1, n):
            total = total + terms[g, i].astype(F32)
        h = (h_ref[rows, :] + total).astype(BF16).astype(F32)
        h_ref[rows, :] = h
        normed(h, 1, normed_ref, pl.ds(pl.multiple_of(lax.rem(g, 2) * G, G), G))

        @pl.when(lax.rem(g, 2) == 1)
        def _():
            a_ref[pl.ds(pl.multiple_of((g - 1) * G, 2 * G), 2 * G), :] = normed_ref[...].astype(BF16)

    pl.semaphore_wait(barrier, n - 1)
    keys(0).wait()
    s_ref[...] = scores(0)

    @pl.loop(0, batch)
    def _(b):
        @pl.when(b + AHEAD < batch)
        def _():
            keys(b + AHEAD).start()
            values(b + AHEAD).start()

        @pl.when(b < no)
        def _():
            pltpu.make_async_copy(
                wo_hbm.at[:, pl.ds(pl.multiple_of(b * T, T), T)], tiles.at[2 * NB + b], wo_sem.at[b]
            ).start()

        @pl.when(b >= batch - AHEAD)
        def _():
            for i in range(2):
                start(gate_up(2 * (b - (batch - AHEAD)) + i, wq_at + 2 * (b - (batch - AHEAD)) + i))

        values(b).wait()

        @pl.when(b + 1 < batch)
        def _():
            keys(b + 1).wait()

        later = scores(jnp.minimum(b + 1, batch - 1))
        s = s_ref[...] * HEAD**-0.5
        e = jnp.exp(s - jnp.max(s, -1, keepdims=True))
        w = (e / jnp.sum(e, -1, keepdims=True)).astype(BF16)
        r = lax.dot_general(w, tiles[2 * lax.rem(b, NB) + 1], (((1,), (1,)), ((), ())), preferred_element_type=F32)
        attn_ref[pl.ds(b, 1), :] = jnp.sum(jnp.where(own, r, 0.0), 0, keepdims=True)
        s_ref[...] = later

        @pl.when(lax.rem(b, G) == G - 1)
        def _():
            g = b // G

            @pl.when(g == 0)
            def _():
                wait(wo)

            part = attn_ref[pl.ds(pl.multiple_of(g * G, G), G), :].astype(BF16)
            for i in range(no):
                terms[g, me, :, i * T : (i + 1) * T] = dot(part, tiles[2 * NB + i]).astype(BF16)
            start(sends(g))

            @pl.when(g > 0)
            def _():
                finish(g - 1)

    for j in range(2 * AHEAD, EARLY + 2 * NB + no):
        start(mlp(j))
    finish(groups - 1)

    quarter = T // 4
    held = EARLY + 2 * NB + no
    for c in range(nc):
        js = range(c * nk, (c + 1) * nk)
        for j in js:
            wait(mlp(j))

        def product(i):
            product = sum(few(a_ref[:, k * T : (k + 1) * T], tiles[place[j], :, i * quarter : (i + 1) * quarter]) for k, j in enumerate(js))
            return product[:batch]

        for i in range(2):
            gate, up = product(i), product(2 + i)
            hidden_ref[:, c * half + i * quarter : c * half + (i + 1) * quarter] = (gate * jax.nn.sigmoid(gate) * up).astype(BF16)
        for j in js:
            if j + held < ngu + nd:
                start(mlp(j + held))

    def send(src, dst, send_sem, recv_sem, to):
        return pltpu.make_async_remote_copy(src, dst, send_sem, recv_sem, device_id={"tp": to}, device_id_type=MESH)

    def term(s, t):
        return send(sums.at[s, t], got.at[s, t], s_send.at[s, t], s_recv.at[s, t], peer(turns[t]))

    def columns_of(device, s):
        return pl.ds(pl.multiple_of(device * T + s * half, half), half)

    def shared(s, i, device):
        part = out_ref.at[:, columns_of(device, s)]
        return send(part, part, y_send.at[s, i - 1], y_recv.at[s, i - 1], peer(i))

    def mine(s):
        return [shared(s, i, me) for i in (2, 1, 3)]

    def finished(s):
        total = own_sum[s]
        for t in range(n - 1):
            term(s, t).wait()
            total = total + got[s, t].astype(F32)
        out_ref[:, columns_of(me, s)] = (h_ref[:, columns_of(me, s)] + total).astype(BF16)
        start(mine(s))

    for at, (s, t) in enumerate(order):
        blocks = range(at * nc, (at + 1) * nc)
        for i in blocks:
            down(i).wait()
        for c in range(2):
            total = 0.0
            for r, i in enumerate(blocks):
                j, (rows, _), _ = block(i)
                total += few(hidden_ref[:, r * half : (r + 1) * half], tiles[place[ngu + j], rows, pl.ds(i % 2 * half + c * quarter, quarter)])
            total, to = total[:batch], slice(c * quarter, (c + 1) * quarter)
            if t < n - 1:
                sums[s, t, :, to] = total.astype(BF16)
            else:
                own_sum[s, :, to] = total
        if t < n - 1:
            term(s, t).start()
        if (s, t) == (1, n - 2):
            finished(0)
    finished(1)
    for s in range(2):
        for i in range(1, n):
            shared(s, i, source(i)).wait_recv()
        for copy in mine(s):
            copy.wait_send()


def solution(mesh):
    n = mesh.shape["tp"]

    def step(x, k_cache, v_cache, gain_a, wq, wo, gain_m, w_gate, w_up, w_down):
        batch, cache, heads, head = k_cache.shape
        d, width = wq.shape
        ff = w_gate.shape[1]
        k = jnp.transpose(k_cache, (0, 2, 3, 1)).reshape(batch, width, cache)
        v = jnp.transpose(v_cache, (0, 2, 3, 1)).reshape(batch, width, cache)
        angle = np.float32(cache - 1) * np.float32(THETA) ** (-np.arange(head // 2, dtype=np.float32) / np.float32(head // 2))
        cos, sin = np.cos(angle), np.sin(angle)
        rot = np.stack([np.tile(np.concatenate(c), heads) for c in ((cos, cos), (-sin, sin))]).astype(np.float32)
        no, nd, ngu = d // T, ff * d // (T * T), 2 * ff * d // (T * T)
        groups = batch // G
        dma = pltpu.SemaphoreType.DMA
        anywhere = pl.BlockSpec(memory_space=pl.ANY)
        return pl.pallas_call(
            functools.partial(kernel, n),
            out_shape=pltpu.VMEM((batch, d), BF16),
            in_specs=[anywhere] * 11,
            out_specs=pl.BlockSpec(memory_space=pltpu.VMEM),
            scratch_shapes=[
                pltpu.VMEM((2 * NB + no + EARLY, T, T), BF16),
                pltpu.VMEM((batch, d), BF16),
                pltpu.VMEM((batch, d), BF16),
                pltpu.VMEM((batch, d), F32),
                pltpu.VMEM((2 * G, d), F32),
                pltpu.VMEM((batch, width), F32),
                pltpu.VMEM((heads, cache), F32),
                pltpu.VMEM((batch, width), F32),
                pltpu.VMEM((2, d // 128, 128), BF16),
                pltpu.VMEM((2, d // 128, 128), F32),
                pltpu.VMEM((2, width), F32),
                pltpu.VMEM((groups, n, G, d), BF16),
                pltpu.VMEM((batch, ff), BF16),
                pltpu.VMEM((2, n - 1, batch, T // 2), BF16),
                pltpu.VMEM((2, batch, T // 2), F32),
                pltpu.VMEM((2, n - 1, batch, T // 2), BF16),
                dma((4,)), dma((d // T,)), dma((NB,)), dma((NB,)), dma((no,)), dma((ngu + nd, 4)),
                dma((groups, n - 1)), dma((groups, n - 1)), dma((2, n - 1)), dma((2, n - 1)), dma((2, n - 1)), dma((2, n - 1)),
            ],
            compiler_params=pltpu.CompilerParams(collective_id=0, has_side_effects=True, vmem_limit_bytes=65011712),
            name="layer",
        )(x, k, v, gain_a.reshape(d // 128, 128), wq, wo, gain_m.reshape(d // 128, 128), w_gate, w_up, w_down, rot)

    states, cache, columns, rows_of = P("dp", None), P("dp", None, "tp", None), P(None, "tp"), P("tp", None)
    return jax.shard_map(
        step,
        mesh=mesh,
        in_specs=(states, cache, cache, P(None), columns, rows_of, P(None), columns, columns, rows_of),
        out_specs=states,
        check_vma=False,
    )
```
